32 devices in a mesh: rows: 8 (over z, y), feat: 4 (over x, core).
Axes of the slice: x: 2, y: 2, z: 4, core: 2. Of those that a mesh axis runs over, the one named last changes fastest.
Arguments:
- features: float32 [100, 8192], P('feat', 'rows'), may hold values from -12 to 12
- tiles: float32 [1024, 128, 128], P('rows'), may hold values from 0 to 1.5
- tile_slot: int32 [1024], P('rows'), may hold values from 0 to 15, as said below
- send_blocks: int32 [8, 8, 1], P('rows'), may hold values from 0 to 7
Outputs:
- ranked: float32 [100, 8192], P('feat', 'rows')
- change: float32 [4], replicated
The draws below stay inside these ranges and needn't reach their ends.
Inputs may be any that keep to these rules, and one draw needn't show every extreme that they name: `tile_slot`: among the tiles of one index of rows, every received slot (8 to 15) is named by at least one tile.
All inputs are finite; a program needn't handle non-finite values.
Results may differ from the reference program's by a relative error of at most 0.0001.
Values sent between devices are 32-bit elements; how exact they have to be, the bound alone decides.
A program may use at most 128 MiB of HBM per device.

```python
import jax
import jax.numpy as jnp
from jax import lax

F = 100
TILE = 128
NB = 8
TPB = 16
SLOTS = 1
ITERS = 4
PEERS = 8
NBLK = 64
NODES = 8192


own_rate = 6.0


halo_rate = 1.5


def slot_plan(key):
    base_key = jax.random.fold_in(key, 7101)
    rank_key, choose_key, local_key, remote_key = jax.random.split(base_key, 4)
    per_device = NB * TPB
    halo_count = PEERS * SLOTS
    ordered = jnp.tile(jnp.arange(per_device, dtype=jnp.int32)[None, :], (PEERS, 1))
    ranking = jax.random.permutation(rank_key, ordered, axis=1, independent=True)
    chooser = jax.random.randint(choose_key, (PEERS, per_device), 0, 4, dtype=jnp.int32)
    local_pick = jax.random.randint(local_key, (PEERS, per_device), 0, NB, dtype=jnp.int32)
    remote_pick = jax.random.randint(remote_key, (PEERS, per_device), NB, NB + halo_count, dtype=jnp.int32)
    drawn_slot = jnp.where(chooser == 0, remote_pick, local_pick)
    slot_table = jnp.where(ranking < halo_count, NB + ranking, drawn_slot)
    return slot_table.reshape(PEERS * per_device).astype(jnp.int32)


def draw_tile_slot(key, part):
    return slot_plan(key)


def draw_tiles(key, part):
    slot_table = slot_plan(key)
    local_tile = slot_table < NB
    density = jnp.minimum(jnp.where(local_tile, own_rate, halo_rate) / TILE, 0.9)
    mask_key, weight_key = jax.random.split(jax.random.fold_in(key, 7202))
    chance = jax.random.uniform(mask_key, (NBLK * TPB, TILE, TILE), jnp.float32)
    weights = jax.random.uniform(weight_key, (NBLK * TPB, TILE, TILE), jnp.float32, 0.5, 1.5)
    return jnp.where(chance < density[:, None, None], weights, 0.0).astype(jnp.float32)


def draw_features(key, part):
    base_key = jax.random.fold_in(key, 3301)
    noise_key, device_key, block_key, scale_key = jax.random.split(base_key, 4)
    device_part = jnp.repeat(jax.random.normal(device_key, (F, PEERS, 1), jnp.float32), NB, axis=1)
    block_part = jax.random.normal(block_key, (F, NBLK, 1), jnp.float32)
    noise = jax.random.normal(noise_key, (F, NBLK, TILE), jnp.float32)
    values = noise + 1.5 * device_part + 0.7 * block_part
    return jnp.clip(values, -12.0, 12.0).reshape(F, NODES).astype(jnp.float32)


def with_ends(result, key, least, largest):
    dims = result.shape
    spot = [jax.random.randint(jax.random.fold_in(key, axis), (), 0, dims[axis]) for axis in range(len(dims))]
    result = result.at[tuple(spot)].set(least)
    longest = dims.index(max(dims))
    spot[longest] = (spot[longest] + 1) % dims[longest]
    return result.at[tuple(spot)].set(largest)


def setup_inputs(seed: int = 0) -> dict:
    keys = jax.random.split(jax.random.key(seed), 5)
    return {
        "features": draw_features(jax.random.fold_in(keys[4], 71), 0),
        "tiles": draw_tiles(jax.random.fold_in(keys[4], 71), 0),
        "tile_slot": draw_tile_slot(jax.random.fold_in(keys[4], 71), 0),
        "send_blocks": with_ends(jax.random.randint(keys[3], (PEERS, PEERS, SLOTS), 0, NB), jax.random.fold_in(keys[3], 1), 0, NB - 1).astype(jnp.int32),
    }


teleport = 0.15


def reference(features, tiles, tile_slot, send_blocks):
    total_tiles = NBLK * TPB
    owner = jnp.arange(total_tiles, dtype=jnp.int32) // (NB * TPB)
    remote = jnp.maximum(tile_slot - NB, 0).astype(jnp.int32)
    source = remote // SLOTS
    within = remote % SLOTS
    column = jnp.where(tile_slot < NB, owner * NB + tile_slot, source * NB + send_blocks[source, owner, within]).astype(jnp.int32)
    degree = 1.0 + jnp.sum(tiles, axis=2).reshape(NBLK, TPB, TILE).sum(axis=1).reshape(NODES)
    current = features
    changes = []
    for iteration in range(ITERS):
        blocks = current.reshape(F, NBLK, TILE)
        picked = blocks[:, column, :]
        product = jnp.einsum("tij,ftj->fti", tiles, picked, precision=lax.Precision.HIGHEST)
        summed = product.reshape(F, NBLK, TPB, TILE).sum(axis=2).reshape(F, NODES)
        updated = (1.0 - teleport) * (current + summed) / degree[None, :] + teleport * features
        changes.append(jnp.sum((updated - current) ** 2) / (F * NODES))
        current = updated
    return current, jnp.stack(changes)
```

```python
import functools

import jax
import jax.numpy as jnp
from jax import lax
from jax.experimental import pallas as pl
from jax.experimental.pallas import tpu as pltpu
from jax.sharding import PartitionSpec as P

ITERS = 4
TELEPORT = 0.15
TRANSPOSED = True
MESH = pl.DeviceIdType.MESH


def split(value):
    high = value.astype(jnp.bfloat16)
    low = (value - high.astype(jnp.float32)).astype(jnp.bfloat16)
    return high, low


def kernel(
    peers, feats, total_count,
    features_ref, tiles_ref, slot_ref, send_ref,
    ranked_ref, change_ref,
    tile_buf, high_buf, low_buf, start, current, inverse, picks, outgoing, halo, change_out, change_in,
    tile_sem, send_sem, recv_sem, change_send_sem, change_recv_sem,
):
    width = features_ref.shape[0]
    blocks, padded, tile = current.shape
    per_block = tiles_ref.shape[0] // blocks
    slots = send_ref.shape[0]
    row = lax.axis_index("rows")
    col = lax.axis_index("feat")
    me = row * feats + col
    devices = peers * feats

    def tile_copy(block):
        part = pl.ds(block * per_block, per_block)
        return pltpu.make_async_copy(tiles_ref.at[part], tile_buf.at[part], tile_sem.at[block])

    for block in range(blocks):
        tile_copy(block).start()

    def greet(step, carry):
        other = lax.rem(me + step, devices)
        pl.semaphore_signal(
            barrier, inc=1, device_id={"rows": other // feats, "feat": lax.rem(other, feats)}, device_id_type=MESH
        )
        return carry

    barrier = pltpu.get_barrier_semaphore()
    lax.fori_loop(1, devices, greet, 0)

    def own_picks(block, value):
        high, low = split(value)
        picks[block, :padded] = high
        picks[block, padded:] = low

    ones_row = lax.broadcasted_iota(jnp.int32, (padded, tile), 0) == width
    for block in range(blocks):
        start[block] = jnp.where(ones_row, 1.0, 0.0)
        start[block, :width] = features_ref[:, block * tile : (block + 1) * tile]
        value = start[block]
        current[block] = value
        own_picks(block, value)

    def halo_copy(iteration, source, target, step):
        return pltpu.make_async_remote_copy(
            src_ref=outgoing.at[iteration, target],
            dst_ref=halo.at[iteration, source],
            send_sem=send_sem.at[iteration, target],
            recv_sem=recv_sem.at[iteration, source],
            device_id={"rows": target},
            device_id_type=MESH,
        )

    def fill(iteration):
        def body(peer, carry):
            for k in range(slots):
                outgoing[iteration, peer, k] = current[send_ref[k, peer]]
            return carry

        lax.fori_loop(0, peers, body, 0)
        for k in range(slots):
            halo[iteration, row, k] = outgoing[iteration, row, k]

    def send(iteration):
        def body(step, carry):
            halo_copy(iteration, row, lax.rem(row + step, peers), step).start()
            return carry

        lax.fori_loop(1, peers, body, 0)

    def receive(iteration):
        def body(step, carry):
            source = lax.rem(row + peers - step, peers)
            halo_copy(iteration, source, source, step).wait_recv()
            return carry

        lax.fori_loop(1, peers, body, 0)

        def unpack(peer, carry):
            for k in range(slots):
                own_picks(blocks + peer * slots + k, halo[iteration, peer, k])
            return carry

        lax.fori_loop(0, peers, unpack, 0)

    def drain(iteration):
        def body(step, carry):
            target = lax.rem(row + step, peers)
            halo_copy(iteration, row, target, step).wait_send()
            return carry

        lax.fori_loop(1, peers, body, 0)

    def product(block):
        gathered = [picks[slot_ref[block * per_block + t]] for t in range(per_block)]
        left = jnp.concatenate(gathered, axis=1)
        if TRANSPOSED:
            dims = (((1,), (0,)), ((), ()))
        else:
            dims = (((1,), (1,)), ((), ()))
        main = lax.dot_general(left, high_buf[block], dims, preferred_element_type=jnp.float32)
        rest = lax.dot_general(left[:padded], low_buf[block], dims, preferred_element_type=jnp.float32)
        return main[:padded] + main[padded:] + rest

    def iterate(iteration, first):
        squares = jnp.zeros((padded, tile), jnp.float32)
        fresh = []
        for block in range(blocks):
            summed = product(block)
            if first:
                scale = (1.0 - TELEPORT) / (1.0 + summed[width : width + 1])
                inverse[block] = jnp.broadcast_to(scale, inverse.shape[1:])
            else:
                scale = inverse[block, :1]
            before = current[block]
            after = (before + summed) * scale + TELEPORT * start[block]
            difference = after - before
            squares = squares + difference * difference
            fresh.append(after)
        for block in range(blocks):
            current[block] = fresh[block]
        feature_row = lax.broadcasted_iota(jnp.int32, (padded, tile), 0) < width
        squares = jnp.sum(jnp.where(feature_row, squares, 0.0))
        lane = lax.broadcasted_iota(jnp.int32, (1, tile), 1)
        return jnp.where(lane == iteration, squares, 0.0)

    fill(0)
    pl.semaphore_wait(barrier, devices - 1)
    send(0)

    for block in range(blocks):
        tile_copy(block).wait()
        for t in range(per_block):
            value = tile_buf[block * per_block + t]
            part = pl.ds(t * tile, tile)
            if TRANSPOSED:
                high, low = split(value.T)
                high_buf[block, part, :] = high
                low_buf[block, part, :] = low
            else:
                high, low = split(value)
                high_buf[block, :, part] = high
                low_buf[block, :, part] = low

    receive(0)
    changes = iterate(0, True)

    def later(iteration, changes):
        fill(iteration)
        send(iteration)
        for block in range(blocks):
            own_picks(block, current[block])
        receive(iteration)
        return changes + iterate(iteration, False)

    changes = lax.fori_loop(1, ITERS, later, changes)
    change_out[0] = changes
    for block in range(blocks):
        ranked_ref[:, block * tile : (block + 1) * tile] = current[block, :width]

    def change_copy(source, target):
        return pltpu.make_async_remote_copy(
            src_ref=change_out.at[0],
            dst_ref=change_in.at[source],
            send_sem=change_send_sem.at[target],
            recv_sem=change_recv_sem.at[source],
            device_id={"rows": target // feats, "feat": lax.rem(target, feats)},
            device_id_type=MESH,
        )

    def share(step, carry):
        change_copy(me, lax.rem(me + step, devices)).start()
        return carry

    lax.fori_loop(1, devices, share, 0)
    change_in[me] = changes
    for iteration in range(ITERS):
        drain(iteration)

    def collect(step, carry):
        source = lax.rem(me + devices - step, devices)
        change_copy(source, source).wait_recv()
        return carry

    lax.fori_loop(1, devices, collect, 0)
    change_ref[...] = jnp.sum(change_in[...], axis=0) * (1.0 / total_count)

    def finish(step, carry):
        target = lax.rem(me + step, devices)
        change_copy(me, target).wait_send()
        return carry

    lax.fori_loop(1, devices, finish, 0)


def solution(mesh):
    peers, feats = mesh.shape["rows"], mesh.shape["feat"]

    def shards(features, tiles, tile_slot, send_blocks):
        width, nodes = features.shape
        tile = tiles.shape[1]
        blocks = nodes // tile
        per_block = tiles.shape[0] // blocks
        slots = send_blocks.shape[2]
        padded = (width // 16 + 1) * 16
        total_count = width * feats * nodes * peers
        depth = per_block * tile
        devices = peers * feats
        split_shape = (blocks, depth, tile) if TRANSPOSED else (blocks, tile, depth)
        vmem = pl.BlockSpec(memory_space=pltpu.VMEM)
        smem = pl.BlockSpec(memory_space=pltpu.SMEM)
        ranked, change = pl.pallas_call(
            functools.partial(kernel, peers, feats, total_count),
            out_shape=(
                jax.ShapeDtypeStruct((width, nodes), jnp.float32),
                jax.ShapeDtypeStruct((1, tile), jnp.float32),
            ),
            in_specs=[vmem, pl.BlockSpec(memory_space=pl.ANY), smem, smem],
            out_specs=(vmem, vmem),
            scratch_shapes=[
                pltpu.VMEM(tiles.shape, jnp.float32),
                pltpu.VMEM(split_shape, jnp.bfloat16),
                pltpu.VMEM(split_shape, jnp.bfloat16),
                pltpu.VMEM((blocks, padded, tile), jnp.float32),
                pltpu.VMEM((blocks, padded, tile), jnp.float32),
                pltpu.VMEM((blocks, 8, tile), jnp.float32),
                pltpu.VMEM((blocks + peers * slots, 2 * padded, tile), jnp.bfloat16),
                pltpu.VMEM((ITERS, peers, slots, padded, tile), jnp.float32),
                pltpu.VMEM((ITERS, peers, slots, padded, tile), jnp.float32),
                pltpu.VMEM((1, 1, tile), jnp.float32),
                pltpu.VMEM((devices, 1, tile), jnp.float32),
                pltpu.SemaphoreType.DMA((blocks,)),
                pltpu.SemaphoreType.DMA((ITERS, peers)),
                pltpu.SemaphoreType.DMA((ITERS, peers)),
                pltpu.SemaphoreType.DMA((devices,)),
                pltpu.SemaphoreType.DMA((devices,)),
            ],
            compiler_params=pltpu.CompilerParams(collective_id=0, has_side_effects=True),
        )(features, tiles, tile_slot, send_blocks[0].T)
        return ranked, change[0, :ITERS]

    return jax.shard_map(
        shards,
        mesh=mesh,
        in_specs=(P("feat", "rows"), P("rows", None, None), P("rows"), P("rows", None, None)),
        out_specs=(P("feat", "rows"), P()),
        check_vma=False,
    )
```

```python
import functools

import jax
import jax.numpy as jnp
from jax import lax
from jax.experimental import pallas as pl
from jax.experimental.pallas import tpu as pltpu
from jax.sharding import PartitionSpec as P

ITERS = 4
TELEPORT = 0.15
TRANSPOSED = True
MESH = pl.DeviceIdType.MESH


def split(value):
    high = value.astype(jnp.bfloat16)
    low = (value - high.astype(jnp.float32)).astype(jnp.bfloat16)
    return high, low


def kernel(
    peers, feats, total_count,
    features_hbm, tiles_ref, slot_hbm, send_hbm,
    ranked_ref, change_ref,
    features_ref, slot_ref, send_ref, input_sem, tile_buf, high_buf, low_buf, start, current, inverse, picks, outgoing, halo, change_out, change_in,
    tile_sem, send_sem, recv_sem, change_send_sem, change_recv_sem,
):
    width = features_ref.shape[0]
    blocks, padded, tile = current.shape
    per_block = tiles_ref.shape[0] // blocks
    slots = send_ref.shape[0]
    row = lax.axis_index("rows")
    col = lax.axis_index("feat")
    me = row * feats + col
    devices = peers * feats
    half = peers // 2
    upper = row // half
    near_count = peers - half

    def tile_copy(block):
        part = pl.ds(block * per_block, per_block)
        return pltpu.make_async_copy(tiles_ref.at[part], tile_buf.at[part], tile_sem.at[block])

    inputs = [
        pltpu.make_async_copy(features_hbm, features_ref, input_sem.at[0]),
        pltpu.make_async_copy(send_hbm, send_ref, input_sem.at[1]),
        pltpu.make_async_copy(slot_hbm, slot_ref, input_sem.at[2]),
    ]
    for copy in inputs:
        copy.start()

    def greet(step, carry):
        other = lax.rem(row + step, peers)
        pl.semaphore_signal(barrier, inc=1, device_id={"rows": other}, device_id_type=MESH)
        return carry

    barrier = pltpu.get_barrier_semaphore()
    lax.fori_loop(1, peers, greet, 0)
    for step in range(1, feats):
        other = lax.rem(col + step, feats)
        pl.semaphore_signal(barrier, inc=1, device_id={"feat": other}, device_id_type=MESH)
    for block in range(blocks):
        tile_copy(block).start()
    for copy in inputs:
        copy.wait()

    def own_picks(block, value):
        high, low = split(value)
        picks[block, :padded] = high
        picks[block, padded:] = low

    tail = jnp.where(lax.broadcasted_iota(jnp.int32, (padded - width, tile), 0) == 0, 1.0, 0.0)
    ones_row = lax.broadcasted_iota(jnp.int32, (padded, tile), 0) == width
    for block in range(blocks):
        start[block] = jnp.where(ones_row, 1.0, 0.0)
        start[block, :width] = features_ref[:, block * tile : (block + 1) * tile]
        value = start[block]
        current[block] = value
        own_picks(block, value)

    def halo_copy(iteration, source, target):
        return pltpu.make_async_remote_copy(
            src_ref=outgoing.at[iteration, target],
            dst_ref=halo.at[iteration, source],
            send_sem=send_sem.at[iteration, target],
            recv_sem=recv_sem.at[iteration, source],
            device_id={"rows": target},
            device_id_type=MESH,
        )

    def fill(iteration):
        def body(peer, carry):
            for k in range(slots):
                outgoing[iteration, peer, k] = current[send_ref[k, peer], :width]
            return carry

        lax.fori_loop(0, peers, body, 0)
        for k in range(slots):
            halo[iteration, row, k] = outgoing[iteration, row, k]

    def send(iteration):
        def across(step, carry):
            far = step + (1 - upper) * (peers - 1 - 2 * step)
            halo_copy(iteration, row, far).start()
            return carry

        def beside(step, carry):
            near = upper * half + lax.rem(row - upper * half + step, near_count)
            halo_copy(iteration, row, near).start()
            return carry

        lax.fori_loop(0, half, across, 0)
        lax.fori_loop(1, near_count, beside, 0)

    def receive(iteration):
        def body(step, carry):
            source = lax.rem(row + peers - step, peers)
            halo_copy(iteration, source, source).wait_recv()
            return carry

        lax.fori_loop(1, peers, body, 0)
        for peer in range(peers):
            for k in range(slots):
                high, low = split(jnp.concatenate([halo[iteration, peer, k], tail], axis=0))
                picks[blocks + peer * slots + k, :padded] = high
                picks[blocks + peer * slots + k, padded:] = low

    def drain(iteration):
        def body(step, carry):
            target = lax.rem(row + step, peers)
            halo_copy(iteration, row, target).wait_send()
            return carry

        lax.fori_loop(1, peers, body, 0)

    def product(block):
        gathered = [picks[slot_ref[block * per_block + t]] for t in range(per_block)]
        left = jnp.concatenate(gathered, axis=1)
        if TRANSPOSED:
            dims = (((1,), (0,)), ((), ()))
        else:
            dims = (((1,), (1,)), ((), ()))
        main = lax.dot_general(left, high_buf[block], dims, preferred_element_type=jnp.float32)
        rest = lax.dot_general(left[:padded], low_buf[block], dims, preferred_element_type=jnp.float32)
        return main[:padded] + main[padded:] + rest

    def iterate(iteration, first):
        squares = jnp.zeros((padded, tile), jnp.float32)
        fresh = []
        for block in range(blocks):
            summed = product(block)
            if first:
                scale = (1.0 - TELEPORT) / (1.0 + summed[width : width + 1])
                inverse[block] = jnp.broadcast_to(scale, inverse.shape[1:])
            else:
                scale = inverse[block, :1]
            before = current[block]
            after = (before + summed) * scale + TELEPORT * start[block]
            difference = after - before
            squares = squares + difference * difference
            fresh.append(after)
        for block in range(blocks):
            current[block] = fresh[block]
        feature_row = lax.broadcasted_iota(jnp.int32, (padded, tile), 0) < width
        squares = jnp.sum(jnp.where(feature_row, squares, 0.0))
        lane = lax.broadcasted_iota(jnp.int32, (1, tile), 1)
        return jnp.where(lane == iteration, squares, 0.0)

    fill(0)
    pl.semaphore_wait(barrier, peers + feats - 2)
    send(0)

    for block in range(blocks):
        tile_copy(block).wait()
        for t in range(per_block):
            value = tile_buf[block * per_block + t]
            part = pl.ds(t * tile, tile)
            if TRANSPOSED:
                high, low = split(value.T)
                high_buf[block, part, :] = high
                low_buf[block, part, :] = low
            else:
                high, low = split(value)
                high_buf[block, :, part] = high
                low_buf[block, :, part] = low

    receive(0)
    changes = iterate(0, True)

    def later(iteration, changes):
        fill(iteration)
        send(iteration)
        for block in range(blocks):
            own_picks(block, current[block])
        receive(iteration)
        return changes + iterate(iteration, False)

    changes = lax.fori_loop(1, ITERS, later, changes)
    change_out[0] = changes
    for block in range(blocks):
        ranked_ref[:, block * tile : (block + 1) * tile] = current[block, :width]

    def change_copy(source, target):
        return pltpu.make_async_remote_copy(
            src_ref=change_out.at[0],
            dst_ref=change_in.at[source],
            send_sem=change_send_sem.at[target],
            recv_sem=change_recv_sem.at[source],
            device_id={"rows": target // feats, "feat": lax.rem(target, feats)},
            device_id_type=MESH,
        )

    def share(step, carry):
        change_copy(me, lax.rem(me + step, devices)).start()
        return carry

    lax.fori_loop(1, devices, share, 0)
    change_in[me] = changes
    for iteration in range(ITERS):
        drain(iteration)

    def collect(step, carry):
        source = lax.rem(me + devices - step, devices)
        change_copy(source, source).wait_recv()
        return carry

    lax.fori_loop(1, devices, collect, 0)
    change_ref[...] = jnp.sum(change_in[...], axis=0) * (1.0 / total_count)

    def finish(step, carry):
        target = lax.rem(me + step, devices)
        change_copy(me, target).wait_send()
        return carry

    lax.fori_loop(1, devices, finish, 0)


def finish_kernel(ranked_in, change_in, ranked_ref, change_ref):
    ranked_ref[...] = ranked_in[...]
    for iteration in range(ITERS):
        change_ref[iteration] = change_in[0, iteration]


def solution(mesh):
    peers, feats = mesh.shape["rows"], mesh.shape["feat"]

    def shards(features, tiles, tile_slot, send_blocks):
        width, nodes = features.shape
        tile = tiles.shape[1]
        blocks = nodes // tile
        per_block = tiles.shape[0] // blocks
        slots = send_blocks.shape[2]
        padded = (width // 16 + 1) * 16
        total_count = width * feats * nodes * peers
        depth = per_block * tile
        devices = peers * feats
        split_shape = (blocks, depth, tile) if TRANSPOSED else (blocks, tile, depth)
        vmem = pl.BlockSpec(memory_space=pltpu.VMEM)
        smem = pl.BlockSpec(memory_space=pltpu.SMEM)
        ranked, change = pl.pallas_call(
            functools.partial(kernel, peers, feats, total_count),
            out_shape=(
                jax.ShapeDtypeStruct((width, nodes), jnp.float32),
                jax.ShapeDtypeStruct((1, tile), jnp.float32),
            ),
            in_specs=[pl.BlockSpec(memory_space=pl.ANY)] * 4,
            out_specs=(vmem, vmem),
            scratch_shapes=[
                pltpu.VMEM(features.shape, jnp.float32),
                pltpu.SMEM(tile_slot.shape, jnp.int32),
                pltpu.SMEM((slots, peers), jnp.int32),
                pltpu.SemaphoreType.DMA((3,)),
                pltpu.VMEM(tiles.shape, jnp.float32),
                pltpu.VMEM(split_shape, jnp.bfloat16),
                pltpu.VMEM(split_shape, jnp.bfloat16),
                pltpu.VMEM((blocks, padded, tile), jnp.float32),
                pltpu.VMEM((blocks, padded, tile), jnp.float32),
                pltpu.VMEM((blocks, 8, tile), jnp.float32),
                pltpu.VMEM((blocks + peers * slots, 2 * padded, tile), jnp.bfloat16),
                pltpu.VMEM((ITERS, peers, slots, width, tile), jnp.float32),
                pltpu.VMEM((ITERS, peers, slots, width, tile), jnp.float32),
                pltpu.VMEM((1, 1, tile), jnp.float32),
                pltpu.VMEM((devices, 1, tile), jnp.float32),
                pltpu.SemaphoreType.DMA((blocks,)),
                pltpu.SemaphoreType.DMA((ITERS, peers)),
                pltpu.SemaphoreType.DMA((ITERS, peers)),
                pltpu.SemaphoreType.DMA((devices,)),
                pltpu.SemaphoreType.DMA((devices,)),
            ],
            compiler_params=pltpu.CompilerParams(collective_id=0, has_side_effects=True),
        )(features, tiles, tile_slot, send_blocks[0].T)
        return pl.pallas_call(
            finish_kernel,
            out_shape=(
                jax.ShapeDtypeStruct((width, nodes), jnp.float32),
                jax.ShapeDtypeStruct((ITERS,), jnp.float32),
            ),
            in_specs=[vmem, smem],
            out_specs=(vmem, smem),
        )(ranked, change)

    return jax.shard_map(
        shards,
        mesh=mesh,
        in_specs=(P("feat", "rows"), P("rows", None, None), P("rows"), P("rows", None, None)),
        out_specs=(P("feat", "rows"), P()),
        check_vma=False,
    )
```

```python
import functools

import jax
import jax.numpy as jnp
from jax import lax
from jax.experimental import pallas as pl
from jax.experimental.pallas import tpu as pltpu
from jax.sharding import PartitionSpec as P

ITERS = 4
TELEPORT = 0.15
TRANSPOSED = True
MESH = pl.DeviceIdType.MESH


def split(value):
    high = value.astype(jnp.bfloat16)
    low = (value - high.astype(jnp.float32)).astype(jnp.bfloat16)
    return high, low


def kernel(
    peers, feats, total_count,
    features_hbm, tiles_ref, slot_hbm, send_hbm,
    ranked_ref, change_ref,
    features_ref, slot_ref, send_ref, input_sem, tile_buf, high_buf, low_buf, start, current, inverse, picks, outgoing, halo, change_out, change_in,
    tile_sem, send_sem, recv_sem, change_send_sem, change_recv_sem,
):
    width = features_ref.shape[0]
    blocks, padded, tile = current.shape
    per_block = tiles_ref.shape[0] // blocks
    slots = send_ref.shape[0]
    row = lax.axis_index("rows")
    col = lax.axis_index("feat")
    me = row * feats + col
    devices = peers * feats
    half = peers // 2
    upper = row // half
    near_count = peers - half

    def tile_copy(block):
        part = pl.ds(block * per_block, per_block)
        return pltpu.make_async_copy(tiles_ref.at[part], tile_buf.at[part], tile_sem.at[block])

    inputs = [
        pltpu.make_async_copy(features_hbm, features_ref, input_sem.at[0]),
        pltpu.make_async_copy(send_hbm, send_ref, input_sem.at[1]),
        pltpu.make_async_copy(slot_hbm, slot_ref, input_sem.at[2]),
    ]
    for copy in inputs:
        copy.start()

    def greet(step, carry):
        other = lax.rem(row + step, peers)
        pl.semaphore_signal(barrier, inc=1, device_id={"rows": other}, device_id_type=MESH)
        return carry

    barrier = pltpu.get_barrier_semaphore()
    lax.fori_loop(1, peers, greet, 0)
    for step in range(1, feats):
        other = lax.rem(col + step, feats)
        pl.semaphore_signal(barrier, inc=1, device_id={"feat": other}, device_id_type=MESH)
    for block in range(blocks):
        tile_copy(block).start()
    for copy in inputs:
        copy.wait()

    def own_picks(block, value):
        high, low = split(value)
        picks[block, :padded] = high
        picks[block, padded:] = low

    tail = jnp.where(lax.broadcasted_iota(jnp.int32, (padded - width, tile), 0) == 0, 1.0, 0.0)
    ones_row = lax.broadcasted_iota(jnp.int32, (padded, tile), 0) == width
    for block in range(blocks):
        start[block] = jnp.where(ones_row, 1.0, 0.0)
        start[block, :width] = features_ref[:, block * tile : (block + 1) * tile]
        value = start[block]
        current[block] = value
        own_picks(block, value)

    def halo_copy(iteration, source, target):
        return pltpu.make_async_remote_copy(
            src_ref=outgoing.at[iteration, target],
            dst_ref=halo.at[iteration, source],
            send_sem=send_sem.at[iteration],
            recv_sem=recv_sem.at[iteration],
            device_id={"rows": target},
            device_id_type=MESH,
        )

    def fill(iteration):
        def body(peer, carry):
            for k in range(slots):
                outgoing[iteration, peer, k] = current[send_ref[k, peer], :width]
            return carry

        lax.fori_loop(0, peers, body, 0)
        for k in range(slots):
            halo[iteration, row, k] = outgoing[iteration, row, k]

    def send(iteration):
        def across(step, carry):
            far = step + (1 - upper) * (peers - 1 - 2 * step)
            halo_copy(iteration, row, far).start()
            return carry

        def beside(step, carry):
            near = upper * half + lax.rem(row - upper * half + step, near_count)
            halo_copy(iteration, row, near).start()
            return carry

        lax.fori_loop(0, half, across, 0)
        lax.fori_loop(1, near_count, beside, 0)

    def receive(iteration):
        landed = halo.at[iteration, pl.ds(0, peers - 1)]
        pltpu.make_async_copy(landed, landed, recv_sem.at[iteration]).wait()
        for peer in range(peers):
            for k in range(slots):
                high, low = split(jnp.concatenate([halo[iteration, peer, k], tail], axis=0))
                picks[blocks + peer * slots + k, :padded] = high
                picks[blocks + peer * slots + k, padded:] = low

    def drain(iteration):
        left = outgoing.at[iteration, pl.ds(0, peers - 1)]
        pltpu.make_async_copy(left, left, send_sem.at[iteration]).wait()

    def product(block):
        gathered = [picks[slot_ref[block * per_block + t]] for t in range(per_block)]
        left = jnp.concatenate(gathered, axis=1)
        if TRANSPOSED:
            dims = (((1,), (0,)), ((), ()))
        else:
            dims = (((1,), (1,)), ((), ()))
        main = lax.dot_general(left, high_buf[block], dims, preferred_element_type=jnp.float32)
        rest = lax.dot_general(left[:padded], low_buf[block], dims, preferred_element_type=jnp.float32)
        return main[:padded] + main[padded:] + rest

    def iterate(iteration, first):
        squares = jnp.zeros((padded, tile), jnp.float32)
        fresh = []
        for block in range(blocks):
            summed = product(block)
            if first:
                scale = (1.0 - TELEPORT) / (1.0 + summed[width : width + 1])
                inverse[block] = jnp.broadcast_to(scale, inverse.shape[1:])
            else:
                scale = inverse[block, :1]
            before = current[block]
            after = (before + summed) * scale + TELEPORT * start[block]
            difference = after - before
            squares = squares + difference * difference
            fresh.append(after)
        for block in range(blocks):
            current[block] = fresh[block]
        feature_row = lax.broadcasted_iota(jnp.int32, (padded, tile), 0) < width
        squares = jnp.sum(jnp.where(feature_row, squares, 0.0))
        lane = lax.broadcasted_iota(jnp.int32, (1, tile), 1)
        return jnp.where(lane == iteration, squares, 0.0)

    fill(0)
    pl.semaphore_wait(barrier, peers + feats - 2)
    send(0)

    for block in range(blocks):
        tile_copy(block).wait()
        for t in range(per_block):
            value = tile_buf[block * per_block + t]
            part = pl.ds(t * tile, tile)
            if TRANSPOSED:
                high, low = split(value.T)
                high_buf[block, part, :] = high
                low_buf[block, part, :] = low
            else:
                high, low = split(value)
                high_buf[block, :, part] = high
                low_buf[block, :, part] = low

    receive(0)
    changes = iterate(0, True)

    def later(iteration, changes):
        fill(iteration)
        send(iteration)
        for block in range(blocks):
            own_picks(block, current[block])
        receive(iteration)
        return changes + iterate(iteration, False)

    changes = lax.fori_loop(1, ITERS, later, changes)
    change_out[0] = changes

    def change_copy(source, target):
        return pltpu.make_async_remote_copy(
            src_ref=change_out.at[0],
            dst_ref=change_in.at[source],
            send_sem=change_send_sem.at[0],
            recv_sem=change_recv_sem.at[0],
            device_id={"rows": target // feats, "feat": lax.rem(target, feats)},
            device_id_type=MESH,
        )

    def share_across(step, carry):
        change_copy(me, step + (1 - upper) * (devices - 1 - 2 * step)).start()
        return carry

    def share_beside(step, carry):
        base = upper * (devices // 2)
        change_copy(me, base + lax.rem(me - base + step, devices - devices // 2)).start()
        return carry

    lax.fori_loop(0, devices // 2, share_across, 0)
    lax.fori_loop(1, devices - devices // 2, share_beside, 0)
    change_in[me] = changes
    for block in range(blocks):
        features_ref[:, block * tile : (block + 1) * tile] = current[block, :width]
    ranked_copy = pltpu.make_async_copy(features_ref, ranked_ref, input_sem.at[0])
    ranked_copy.start()
    for iteration in range(ITERS):
        drain(iteration)

    landed = change_in.at[pl.ds(0, devices - 1)]
    pltpu.make_async_copy(landed, landed, change_recv_sem.at[0]).wait()
    change_ref[...] = jnp.sum(change_in[...], axis=0) * (1.0 / total_count)

    pltpu.make_async_copy(landed, landed, change_send_sem.at[0]).wait()
    ranked_copy.wait()


def finish_kernel(ranked_in, change_in, ranked_ref, change_ref):
    ranked_ref[...] = ranked_in[...]
    for iteration in range(ITERS):
        change_ref[iteration] = change_in[0, iteration]


def solution(mesh):
    peers, feats = mesh.shape["rows"], mesh.shape["feat"]

    def shards(features, tiles, tile_slot, send_blocks):
        width, nodes = features.shape
        tile = tiles.shape[1]
        blocks = nodes // tile
        per_block = tiles.shape[0] // blocks
        slots = send_blocks.shape[2]
        padded = (width // 16 + 1) * 16
        total_count = width * feats * nodes * peers
        depth = per_block * tile
        devices = peers * feats
        split_shape = (blocks, depth, tile) if TRANSPOSED else (blocks, tile, depth)
        vmem = pl.BlockSpec(memory_space=pltpu.VMEM)
        smem = pl.BlockSpec(memory_space=pltpu.SMEM)
        ranked, change = pl.pallas_call(
            functools.partial(kernel, peers, feats, total_count),
            out_shape=(
                jax.ShapeDtypeStruct((width, nodes), jnp.float32),
                jax.ShapeDtypeStruct((1, tile), jnp.float32),
            ),
            in_specs=[pl.BlockSpec(memory_space=pl.ANY)] * 4,
            out_specs=(pl.BlockSpec(memory_space=pl.ANY), vmem),
            scratch_shapes=[
                pltpu.VMEM(features.shape, jnp.float32),
                pltpu.SMEM(tile_slot.shape, jnp.int32),
                pltpu.SMEM((slots, peers), jnp.int32),
                pltpu.SemaphoreType.DMA((3,)),
                pltpu.VMEM(tiles.shape, jnp.float32),
                pltpu.VMEM(split_shape, jnp.bfloat16),
                pltpu.VMEM(split_shape, jnp.bfloat16),
                pltpu.VMEM((blocks, padded, tile), jnp.float32),
                pltpu.VMEM((blocks, padded, tile), jnp.float32),
                pltpu.VMEM((blocks, 8, tile), jnp.float32),
                pltpu.VMEM((blocks + peers * slots, 2 * padded, tile), jnp.bfloat16),
                pltpu.VMEM((ITERS, peers, slots, width, tile), jnp.float32),
                pltpu.VMEM((ITERS, peers, slots, width, tile), jnp.float32),
                pltpu.VMEM((1, 1, tile), jnp.float32),
                pltpu.VMEM((devices, 1, tile), jnp.float32),
                pltpu.SemaphoreType.DMA((blocks,)),
                pltpu.SemaphoreType.DMA((ITERS,)),
                pltpu.SemaphoreType.DMA((ITERS,)),
                pltpu.SemaphoreType.DMA((1,)),
                pltpu.SemaphoreType.DMA((1,)),
            ],
            compiler_params=pltpu.CompilerParams(collective_id=0, has_side_effects=True),
        )(features, tiles, tile_slot, send_blocks[0].T)
        return pl.pallas_call(
            finish_kernel,
            out_shape=(
                jax.ShapeDtypeStruct((width, nodes), jnp.float32),
                jax.ShapeDtypeStruct((ITERS,), jnp.float32),
            ),
            in_specs=[vmem, smem],
            out_specs=(vmem, smem),
        )(ranked, change)

    return jax.shard_map(
        shards,
        mesh=mesh,
        in_specs=(P("feat", "rows"), P("rows", None, None), P("rows"), P("rows", None, None)),
        out_specs=(P("feat", "rows"), P()),
        check_vma=False,
    )
```
